32 devices in a mesh: nodes: 32 (over z, y, x, core).
Axes of the slice: x: 2, y: 2, z: 4, core: 2. Of those that a mesh axis runs over, the one named last changes fastest.
Arguments:
- adjacency: bfloat16 [16384, 16384], P('nodes')
- features: bfloat16 [16384, 602], P('nodes')
- w_one: float32 [602, 256], replicated
- w_two: float32 [256, 41], replicated
- labels: int32 [16384], P('nodes')
- label_mask: int32 [16384], P('nodes')
Outputs:
- output 1: float32 [1], replicated
- output 2: float32 [602, 256], replicated
- output 3: float32 [256, 41], replicated
All inputs are finite; a program needn't handle non-finite values.
Results may differ from the reference program's by a relative error of at most 0.001.
Values are sent between devices in bfloat16 or wider.
A program may use at most 1 GiB of HBM per device.

```python
import math
import jax
import jax.numpy as jnp
from jax import lax

NODES = 16384
BLOCK_ROWS = 512
F_IN = 602
HIDDEN = 256
CLASSES = 41

ROW_CONTRACT = (((0,), (0,)), ((), ()))
COL_CONTRACT = (((1,), (1,)), ((), ()))


def setup_inputs(seed: int = 0) -> dict:
    key_list = jax.random.split(jax.random.key(seed), 8)
    num_comms = NODES // BLOCK_ROWS
    shifts = jax.random.randint(key_list[0], (2,), 1, num_comms)
    col_ids = jnp.arange(NODES)
    col_comm = col_ids // BLOCK_ROWS
    row_ids = jnp.arange(BLOCK_ROWS)

    def draw_rows(block_idx):
        hot_cols = (col_comm == (block_idx + shifts[0]) % num_comms) | (col_comm == (block_idx + shifts[1]) % num_comms)
        edge_prob = jnp.where(hot_cols, 0.5, 0.01)
        coin_flip = jax.random.uniform(jax.random.fold_in(key_list[1], block_idx), (BLOCK_ROWS, NODES))
        self_loop = col_ids[None, :] == block_idx * BLOCK_ROWS + row_ids[:, None]
        raw_edges = jnp.where((coin_flip < edge_prob[None, :]) | self_loop, 1.0, 0.0)
        return (raw_edges / jnp.sum(raw_edges, axis=1, keepdims=True)).astype(jnp.bfloat16)

    adjacency = lax.map(draw_rows, jnp.arange(num_comms)).reshape(NODES, NODES)
    centers = jax.random.normal(key_list[2], (num_comms, F_IN))
    feat_noise = jax.random.normal(key_list[3], (NODES, F_IN))
    features = (jnp.repeat(centers, BLOCK_ROWS, axis=0) + feat_noise).astype(jnp.bfloat16)
    w_one = jax.random.normal(key_list[4], (F_IN, HIDDEN)) * math.sqrt(2.0 / F_IN)
    w_two = jax.random.normal(key_list[5], (HIDDEN, CLASSES)) * (2.0 / math.sqrt(HIDDEN))
    labels = jax.random.randint(key_list[6], (NODES,), 0, CLASSES, dtype=jnp.int32)
    drawn_mask = jax.random.randint(key_list[7], (NODES,), 0, 10, dtype=jnp.int32) < 3
    label_mask = jnp.where((jnp.arange(NODES) % 10 == 0) | drawn_mask, 1, 0).astype(jnp.int32)
    return {'adjacency': adjacency, 'features': features, 'w_one': w_one.astype(jnp.float32), 'w_two': w_two.astype(jnp.float32), 'labels': labels, 'label_mask': label_mask}


def reference(adjacency, features, w_one, w_two, labels, label_mask):
    weight_one = w_one.astype(jnp.bfloat16)
    weight_two = w_two.astype(jnp.bfloat16)
    agg_one = jnp.dot(adjacency, features, preferred_element_type=jnp.float32).astype(jnp.bfloat16)
    pre_one = jnp.dot(agg_one, weight_one, preferred_element_type=jnp.float32)
    hidden = jnp.maximum(pre_one, 0.0).astype(jnp.bfloat16)
    agg_two = jnp.dot(adjacency, hidden, preferred_element_type=jnp.float32).astype(jnp.bfloat16)
    logits = jnp.dot(agg_two, weight_two, preferred_element_type=jnp.float32)
    weight = label_mask.astype(jnp.float32)
    label_count = jnp.sum(weight)
    onehot = (labels[:, None] == jnp.arange(CLASSES)[None, :]).astype(jnp.float32)
    log_prob = jax.nn.log_softmax(logits, axis=-1)
    loss_value = -jnp.sum(weight * jnp.sum(onehot * log_prob, axis=-1)) / label_count
    grad_two = (weight[:, None] * (jnp.exp(log_prob) - onehot) / label_count).astype(jnp.bfloat16)
    dw_two = lax.dot_general(agg_two, grad_two, ROW_CONTRACT, preferred_element_type=jnp.float32)
    back_two = lax.dot_general(grad_two, weight_two, COL_CONTRACT, preferred_element_type=jnp.float32).astype(jnp.bfloat16)
    d_hidden = lax.dot_general(adjacency, back_two, ROW_CONTRACT, preferred_element_type=jnp.float32)
    grad_one = jnp.where(pre_one > 0.0, d_hidden, 0.0).astype(jnp.bfloat16)
    dw_one = lax.dot_general(agg_one, grad_one, ROW_CONTRACT, preferred_element_type=jnp.float32)
    return (loss_value.reshape(1), dw_one, dw_two)
```

```python
import functools

import jax
import jax.numpy as jnp
from jax import lax
from jax.experimental import pallas as pl
from jax.experimental.pallas import tpu as pltpu
from jax.sharding import PartitionSpec as P

AXIS = 'nodes'
MESH = pl.DeviceIdType.MESH
NN = (((1,), (0,)), ((), ()))
NT = (((1,), (1,)), ((), ()))
COL, CW, CCW, OA, OB, OZ = range(6)
VMEM_BYTES = 62 * 1024 * 1024


def _dot(a, b, dims=NN):
    return lax.dot_general(a, b, dims, preferred_element_type=jnp.float32)


def _ring(v):
    return v + v // 2 - 2 * (v // 3)


class _Geo:
    def __init__(self):
        self.me = lax.axis_index(AXIS)
        self.c = lax.rem(self.me, 2)
        chip = self.me // 2
        self.z = chip // 4
        self.r = _ring(lax.rem(chip, 4))
        self.nxt = lax.rem(self.r + 1, 4)
        self.prv = lax.rem(self.r + 3, 4)
        self.opp = lax.rem(self.r + 2, 4)
        self.other = 1 - self.c
        flip = self.z // 2
        zz = self.z + flip * (3 - 2 * self.z)
        first = 1 - zz
        self.k = [first + flip * (3 - 2 * first)] + [v + flip * (3 - 2 * v) for v in (2, 3)]

    def chip(self, z, r):
        return z * 4 + _ring(r)

    def dev(self, z, r, c):
        return self.chip(z, r) * 2 + c

    def away(self, z0):
        return self.z + 2 * (z0 < self.z).astype(jnp.int32) - 1

    def toward(self, z0):
        return self.z - 2 * (z0 < self.z).astype(jnp.int32) + 1


def _inside(z):
    return jnp.logical_and(z >= 0, z <= 3)


def _rcopy(src, dst, send_sem, recv_sem, dev):
    return pltpu.make_async_remote_copy(src_ref=src, dst_ref=dst, send_sem=send_sem, recv_sem=recv_sem, device_id=(dev,), device_id_type=MESH)


class _Sends:
    def __init__(self):
        self.pending = []

    def start(self, copy, cond=None):
        if cond is None:
            copy.start()
        else:
            @pl.when(cond)
            def _():
                copy.start()
        self.pending.append((copy, cond))

    def finish(self):
        for copy, cond in self.pending:
            if cond is None:
                copy.wait_send()
            else:
                @pl.when(cond)
                def _():
                    copy.wait_send()


def _barrier(g, far):
    sem = pltpu.get_barrier_semaphore()

    def signal(dev):
        pl.semaphore_signal(sem, inc=1, device_id=(dev,), device_id_type=MESH)

    for dev in (g.dev(g.z, g.r, g.other), g.dev(g.z, g.nxt, g.c), g.dev(g.z, g.prv, g.c)):
        signal(dev)
    if far:
        signal(g.dev(g.z, g.opp, g.c))
        for z0 in g.k:
            signal(g.dev(z0, g.r, g.c))
        pl.semaphore_wait(sem, 7)
    else:
        @pl.when(g.z < 3)
        def _():
            signal(g.dev(g.z + 1, g.r, g.c))

        @pl.when(g.z > 0)
        def _():
            signal(g.dev(g.z - 1, g.r, g.c))

        pl.semaphore_wait(sem, 5 - (g.z < 1).astype(jnp.int32) - (g.z > 2).astype(jnp.int32))


def _gather(g, buf, rows, unit, rsem, ssem, consume, early=None):
    ra = -(-rows * 5 // 32 // unit) * unit
    parts = {OA: (0, ra), OB: (ra, ra), OZ: (2 * ra, rows - 2 * ra)}
    ha = rows // 2 // unit * unit
    halves = {OA: (0, ha), OB: (ha, rows - ha)}
    z, r, c = g.z, g.r, g.c
    column = {COL: r, CW: g.prv, CCW: g.nxt, OA: g.opp, OB: g.opp, OZ: g.opp}
    sends = _Sends()

    def piece(kind, z0, core, same):
        ref = buf.at[g.dev(z0, column[kind], core)]
        if kind in (OA, OB):
            ref = ref.at[pl.ds(*(halves if same else parts)[kind]), :]
        elif kind == OZ:
            ref = ref.at[pl.ds(*parts[OZ]), :]
        return ref

    def recv(kind, z0, same=False, partner=False):
        core = g.other if partner else c
        ref = piece(kind, z0, core, same)
        sem = rsem.at[((1 if partner else 0) * 6 + kind) * 4 + z0]
        _rcopy(ref, ref, ssem.at[0], sem, g.me).wait_recv()

    def send(ref, kind, z0, slot, dev, cond=None, partner=False):
        sem = rsem.at[((1 if partner else 0) * 6 + kind) * 4 + z0]
        sends.start(_rcopy(ref, ref, ssem.at[slot * 4 + z0], sem, dev), cond)

    def to_partner(kind, z0, slot, same=False):
        send(piece(kind, z0, c, same), kind, z0, slot, g.dev(z, r, g.other), partner=True)

    def forward_col(z0):
        ref = piece(COL, z0, c, False)
        nz = g.away(z0)
        send(ref, COL, z0, 0, g.dev(nz, r, c), _inside(nz))
        send(ref, CW, z0, 2, g.dev(z, g.nxt, c))
        send(ref, CCW, z0, 3, g.dev(z, g.prv, c))
        to_partner(COL, z0, 4)

    def forward_sides(z0, same=False):
        sub = halves if same else parts
        send(piece(CW, z0, c, same).at[pl.ds(*sub[OA]), :], OA, z0, 5, g.dev(z, g.nxt, c))
        send(piece(CCW, z0, c, same).at[pl.ds(*sub[OB]), :], OB, z0, 7, g.dev(z, g.prv, c))
        to_partner(CW, z0, 6)
        to_partner(CCW, z0, 8)

    def take_opp(z0, same=False):
        kinds = ((OA, 9), (OB, 10)) + (() if same else ((OZ, 11),))
        if not same:
            recv(OZ, z0)
            nz = g.away(z0)
            send(piece(OZ, z0, c, False), OZ, z0, 12, g.dev(nz, r, c), _inside(nz))
            to_partner(OZ, z0, 11)
        for kind, slot in kinds[:2]:
            recv(kind, z0, same)
            to_partner(kind, z0, slot, same)

    def take_col(z0):
        recv(COL, z0)
        forward_col(z0)

    def take_sides(z0, same=False):
        recv(CW, z0, same)
        recv(CCW, z0, same)
        forward_sides(z0, same)

    def pair(kind, z0, same=False, wait_partner=True):
        if wait_partner:
            kinds = (kind,) if kind != OZ else ((OA, OB) if same else (OA, OB, OZ))
            for one in kinds:
                recv(one, z0, same, partner=True)
        consume(g.chip(z0, column[kind]))

    own = buf.at[g.me]
    send(own, COL, z, 0, g.dev(z + 1, r, c), z < 3)
    send(own, COL, z, 1, g.dev(z - 1, r, c), z > 0)
    send(own, CW, z, 2, g.dev(z, g.nxt, c))
    send(own, CCW, z, 3, g.dev(z, g.prv, c))
    send(own, COL, z, 4, g.dev(z, r, g.other), partner=True)
    if early is not None:
        early()
    k0, k1, k2 = g.k
    pair(COL, z)
    take_sides(z, True)
    take_col(k0)
    take_col(k1)
    pair(CW, z)
    pair(CCW, z)
    take_opp(z, True)
    oz = piece(OZ, z, c, False)
    late = g.away(k2)
    send(oz, OZ, z, 12, g.dev(2 * z - late, r, c), _inside(2 * z - late))
    pair(COL, k0)
    take_sides(k0)
    pair(COL, k1)
    take_col(k2)
    send(oz, OZ, z, 13, g.dev(late, r, c), _inside(late))
    pair(CW, k0)
    pair(CCW, k0)
    pair(OZ, z, True)
    take_sides(k1)
    pair(COL, k2)
    take_opp(k0)
    pair(CW, k1)
    pair(CCW, k1)
    take_sides(k2)
    pair(OZ, k0)
    take_opp(k1)
    pair(CW, k2)
    pair(CCW, k2)
    take_opp(k2)
    pair(OZ, k1)
    pair(OZ, k2)
    return sends


def _layer_one(nodes_block, feats, adj, own_x, w_one_t, s1_out, pos_out, h_out, cnt_out, a_v, x_all, acc, cnt, rsem, ssem, lsem):
    g = _Geo()
    load_x = pltpu.make_async_copy(own_x, x_all.at[g.me], lsem.at[0])
    load_a = pltpu.make_async_copy(adj, a_v, lsem.at[1])
    load_x.start()
    load_a.start()
    acc[...] = jnp.zeros_like(acc)
    cnt[...] = jnp.zeros_like(cnt)
    _barrier(g, False)
    load_x.wait()

    def consume(chip):
        def one(core, carry):
            b = chip * 2 + core
            a_blk = a_v[:, pl.ds(pl.multiple_of(b * nodes_block, nodes_block), nodes_block)]
            acc[...] += _dot(x_all[b], a_blk, NT)
            cnt[...] += x_all[b, pl.ds(feats // 16 * 16, 16), :].astype(jnp.float32)
            return carry

        lax.fori_loop(0, 2, one, 0)

    rows = x_all.shape[1]
    sends = _gather(g, x_all, rows, 16, rsem, ssem, consume, load_a.wait)
    s1 = acc[...].astype(jnp.bfloat16)
    s1_out[...] = s1
    pre = _dot(w_one_t[...], s1)
    pos_out[...] = jnp.where(pre > 0.0, 1.0, 0.0)
    h_out[...] = jnp.maximum(pre, 0.0).astype(jnp.bfloat16)
    row = lax.broadcasted_iota(jnp.int32, cnt.shape, 0) == feats % 16
    cnt_out[...] = jnp.broadcast_to(jnp.sum(jnp.where(row, cnt[...], 0.0), keepdims=True), cnt_out.shape)
    sends.finish()


def _layer_two(nodes_block, classes, adj, own_h, s1, pos, count, w_two_t, w_two, labels, mask, out,
               a_v, a_p, h_all, acc, ut, part, pa, pb, fl, fr, cz, oz, red, mine, got_l, got_z, quart,
               rsem, ssem, lsem, xsem, qrs, qss, trs, tss):
    g = _Geo()
    z, r, c = g.z, g.r, g.c
    k0, k1, k2 = g.k
    load_h = pltpu.make_async_copy(own_h, h_all.at[g.me], lsem.at[0])
    load_a = pltpu.make_async_copy(adj, a_v, lsem.at[1])
    load_h.start()
    load_a.start()
    acc[...] = jnp.zeros_like(acc)
    _barrier(g, True)
    load_h.wait()
    partner = g.dev(z, r, g.other)

    def cols(b):
        return pl.ds(pl.multiple_of(b * nodes_block, nodes_block), nodes_block)

    def swap(q):
        return _rcopy(adj.at[:, cols(q * 2 + g.other)], a_p.at[q], xsem.at[0], xsem.at[1], partner)

    def early():
        def one(q, carry):
            swap(q).start()
            return carry

        lax.fori_loop(0, 16, one, 0)
        load_a.wait()

    def consume(chip):
        def one(core, carry):
            b = chip * 2 + core
            acc[...] += _dot(h_all[b], a_v[:, cols(b)], NT)
            return carry

        lax.fori_loop(0, 2, one, 0)

    hidden = h_all.shape[1]
    sends = _gather(g, h_all, hidden, 16, rsem, ssem, consume, early)

    s2 = acc[...].astype(jnp.bfloat16)
    logits = _dot(w_two_t[...], s2)
    weight = mask[...].astype(jnp.float32)
    onehot = (labels[...] == lax.broadcasted_iota(jnp.int32, logits.shape, 0)).astype(jnp.float32)
    shifted = logits - jnp.max(logits, axis=0, keepdims=True)
    log_prob = shifted - jnp.log(jnp.sum(jnp.exp(shifted), axis=0, keepdims=True))
    g2 = (weight * (jnp.exp(log_prob) - onehot) / count[0:1, 0:1]).astype(jnp.bfloat16)
    ut[0] = _dot(w_two[...], g2).astype(jnp.bfloat16)
    send_u = _rcopy(ut.at[0], ut.at[1], xsem.at[2], xsem.at[3], partner)
    send_u.start()
    loss = -jnp.sum(weight * jnp.sum(onehot * log_prob, axis=0, keepdims=True), keepdims=True)
    feats_rows = s1.shape[0]
    extra = red.shape[0] - feats_rows
    dw2 = _dot(g2, s2, NT)
    red[pl.ds(feats_rows, classes), :] = dw2
    red[pl.ds(feats_rows + classes, extra - classes), :] = jnp.broadcast_to(loss, (extra - classes, hidden))
    _rcopy(a_p, a_p, xsem.at[0], xsem.at[1], partner).wait_recv()
    send_u.wait_recv()

    def make(z0, column):
        q = g.chip(z0, column)
        part[q] = _dot(ut[0], a_v[:, cols(q * 2 + c)]) + _dot(ut[1], a_p[q])

    ra = -(-hidden * 5 // 32 // 8) * 8
    parts = {OA: (0, ra), OB: (ra, ra), OZ: (2 * ra, hidden - 2 * ra)}
    halves = {OA: (0, hidden // 2), OB: (hidden // 2, hidden // 2)}
    rs = _Sends()

    def rsend(src, dst, slot, index, recv_index, dev, cond=None):
        rs.start(_rcopy(src, dst, qss.at[slot * 4 + index], qrs.at[recv_index], dev), cond)

    def rwait(ref, index):
        _rcopy(ref, ref, qss.at[0], qrs.at[index], g.me).wait_recv()

    def out_opp(z0, same=False):
        sub = halves if same else parts
        blk = part.at[g.chip(z0, g.opp)]
        rsend(blk.at[pl.ds(*sub[OA]), :], pa.at[z0, pl.ds(0, sub[OA][1]), :], 0, z0, z0, g.dev(z, g.prv, c))
        rsend(blk.at[pl.ds(*sub[OB]), :], pb.at[z0, pl.ds(0, sub[OB][1]), :], 1, z0, 4 + z0, g.dev(z, g.nxt, c))

    def slot_at(z0, nz):
        end = (nz == z0).astype(jnp.int32) * (nz < z).astype(jnp.int32)
        return z0 + end * (4 - z0)

    def out_opp_z(z0):
        blk = part.at[g.chip(z0, g.opp), pl.ds(*parts[OZ]), :]
        far = g.away(z0)

        @pl.when(_inside(far))
        def _():
            rwait(oz.at[z0], 21 + z0)
            q = g.chip(z0, g.opp)
            part[q, pl.ds(*parts[OZ]), :] += oz[z0]

        nz = g.toward(z0)
        slot = slot_at(z0, nz)
        rsend(blk, oz.at[slot], 2, z0, 21 + slot, g.dev(nz, r, c))

    def out_sides(z0, same=False):
        sub = halves if same else parts
        qp, qn = g.chip(z0, g.prv), g.chip(z0, g.nxt)
        na, nb = sub[OA][1], sub[OB][1]
        rwait(pa.at[z0, pl.ds(0, na), :], z0)
        part[qp, pl.ds(*sub[OA]), :] += pa[z0, pl.ds(0, na), :]
        rsend(part.at[qp], fr.at[z0], 3, z0, 12 + z0, g.dev(z, g.prv, c))
        rwait(pb.at[z0, pl.ds(0, nb), :], 4 + z0)
        part[qn, pl.ds(*sub[OB]), :] += pb[z0, pl.ds(0, nb), :]
        rsend(part.at[qn], fl.at[z0], 4, z0, 8 + z0, g.dev(z, g.nxt, c))

    def add_sides(z0):
        q = g.chip(z0, r)
        rwait(fl.at[z0], 8 + z0)
        rwait(fr.at[z0], 12 + z0)
        part[q] += fl[z0] + fr[z0]

    def add_cz(slot, z0, cond):
        @pl.when(cond)
        def _():
            rwait(cz.at[slot], 16 + slot)
            part[g.chip(z0, r)] += cz[slot]

    def out_col(z0):
        add_sides(z0)
        add_cz(z0, z0, _inside(g.away(z0)))
        nz = g.toward(z0)
        slot = slot_at(z0, nz)
        rsend(part.at[g.chip(z0, r)], cz.at[slot], 5, z0, 16 + slot, g.dev(nz, r, c))

    make(k2, g.opp)
    out_opp(k2)
    make(k1, g.opp)
    out_opp(k1)
    make(k2, g.prv)
    make(k2, g.nxt)
    out_opp_z(k2)
    out_sides(k2)
    make(k0, g.opp)
    out_opp(k0)
    make(k1, g.prv)
    make(k1, g.nxt)
    out_opp_z(k1)
    out_sides(k1)
    make(k2, r)
    make(k0, g.prv)
    make(k0, g.nxt)
    out_opp_z(k0)
    out_sides(k0)
    out_col(k2)
    for column in (g.opp, g.prv, g.nxt, r):
        make(z, column)
    make(k1, r)
    make(k0, r)
    out_col(k1)

    def add_oz(slot, cond):
        @pl.when(cond)
        def _():
            rwait(oz.at[slot], 21 + slot)
            part[g.chip(z, g.opp), pl.ds(*parts[OZ]), :] += oz[slot]

    add_oz(z, z > 0)
    add_oz(4, z < 3)
    out_opp(z, True)
    out_col(k0)
    out_sides(z, True)
    add_sides(z)
    add_cz(z, z, z > 0)
    add_cz(4, z, z < 3)
    d_hidden = part[g.chip(z, r)]
    g1 = jnp.where(pos[...] > 0.0, d_hidden, 0.0).astype(jnp.bfloat16)
    red[pl.ds(0, feats_rows), :] = _dot(s1[...], g1, NT)

    half = hidden // 2
    rows = red.shape[0]
    quarter = rows // 4
    tail = _Sends()

    def tsend(src, dst, index, dev):
        tail.start(_rcopy(src, dst, tss.at[index], trs.at[index], dev))

    def twait(ref, index):
        _rcopy(ref, ref, tss.at[0], trs.at[index], g.me).wait_recv()

    def lanes(core):
        return pl.ds(pl.multiple_of(core * half, half), half)

    def band(place):
        return pl.ds(pl.multiple_of(place * quarter, 8), quarter)

    tsend(red.at[:, lanes(g.other)], mine.at[1], 0, partner)
    twait(mine.at[1], 0)
    mine[0] = red[:, lanes(c)] + mine[1]
    peers = (g.nxt, g.prv, g.opp)
    for i, place in enumerate(peers):
        tsend(mine.at[0, band(place), :], got_l.at[i], 1 + i, g.dev(z, place, c))
    total = mine[0, band(r), :]
    for i in range(3):
        twait(got_l.at[i], 1 + i)
        total = total + got_l[i]
    quart[...] = total
    for i, z0 in enumerate((k0, k1, k2)):
        tail.start(_rcopy(quart, got_z.at[z], tss.at[4 + i], trs.at[4 + z], g.dev(z0, r, c)))
    got_z[z] = quart[...]
    for z0 in g.k:
        twait(got_z.at[z0], 4 + z0)
    out_lanes = out.at[:, lanes(c)]
    final = out_lanes.at[band(r), :]
    out[band(r), lanes(c)] = (got_z[0] + got_z[1]) + (got_z[2] + got_z[3])
    for i, place in enumerate(peers):
        tail.start(_rcopy(final, final, tss.at[8 + i], trs.at[8 + r], g.dev(z, place, c)))
    for place in peers:
        twait(out_lanes.at[band(place), :], 8 + place)
    tail.start(_rcopy(out_lanes, out_lanes, tss.at[12], trs.at[12], partner))
    other = out.at[:, lanes(g.other)]
    twait(other, 12)

    swap_all = _rcopy(a_p, a_p, xsem.at[0], xsem.at[1], partner)
    swap_all.wait_send()
    send_u.wait_send()
    sends.finish()
    rs.finish()
    tail.finish()


def solution(mesh):
    def local_step(adj_rows, feat_rows, w_one, w_two, label_rows, mask_rows):
        block, feats = feat_rows.shape
        hidden, classes = w_two.shape
        devices = mesh.shape[AXIS]
        nodes = adj_rows.shape[1]
        bf16, f32 = jnp.bfloat16, jnp.float32
        pad = -(-(feats + 1) // 16) * 16
        vmem = pl.BlockSpec(memory_space=pltpu.VMEM)
        anywhere = pl.BlockSpec(memory_space=pl.ANY)
        dma = pltpu.SemaphoreType.DMA

        own_x = jnp.concatenate([feat_rows.T, mask_rows.astype(bf16)[None, :], jnp.zeros((pad - feats - 1, block), bf16)], axis=0)
        w_one_t = jnp.concatenate([w_one.astype(bf16).T, jnp.zeros((hidden, pad - feats), bf16)], axis=1)
        s1, pos, h1, count = pl.pallas_call(
            functools.partial(_layer_one, block, feats),
            out_shape=(jax.ShapeDtypeStruct((pad, block), bf16), jax.ShapeDtypeStruct((hidden, block), f32),
                       jax.ShapeDtypeStruct((hidden, block), bf16), jax.ShapeDtypeStruct((8, 128), f32)),
            in_specs=[anywhere, anywhere, vmem],
            out_specs=(vmem, vmem, vmem, vmem),
            scratch_shapes=[
                pltpu.VMEM((block, nodes), bf16), pltpu.VMEM((devices, pad, block), bf16),
                pltpu.VMEM((pad, block), f32), pltpu.VMEM((16, block), f32),
                dma((48,)), dma((56,)), dma((2,)),
            ],
            compiler_params=pltpu.CompilerParams(collective_id=0, has_side_effects=True, vmem_limit_bytes=VMEM_BYTES),
            name='layer_one',
        )(adj_rows, own_x, w_one_t)

        weight_two = w_two.astype(bf16)
        red_rows = -(-(pad + classes + 1) // 32) * 32
        quarter = red_rows // 4
        ra = -(-hidden * 5 // 32 // 8) * 8
        out = pl.pallas_call(
            functools.partial(_layer_two, block, classes),
            out_shape=jax.ShapeDtypeStruct((red_rows, hidden), f32),
            in_specs=[anywhere, anywhere] + [vmem] * 7,
            out_specs=vmem,
            scratch_shapes=[
                pltpu.VMEM((block, nodes), bf16), pltpu.VMEM((16, block, block), bf16),
                pltpu.VMEM((devices, hidden, block), bf16), pltpu.VMEM((hidden, block), f32),
                pltpu.VMEM((2, hidden, block), bf16), pltpu.VMEM((16, hidden, block), f32),
                pltpu.VMEM((4, hidden // 2, block), f32), pltpu.VMEM((4, hidden // 2, block), f32),
                pltpu.VMEM((4, hidden, block), f32), pltpu.VMEM((4, hidden, block), f32),
                pltpu.VMEM((5, hidden, block), f32), pltpu.VMEM((5, hidden - 2 * ra, block), f32),
                pltpu.VMEM((red_rows, hidden), f32), pltpu.VMEM((2, red_rows, hidden // 2), f32),
                pltpu.VMEM((3, quarter, hidden // 2), f32), pltpu.VMEM((4, quarter, hidden // 2), f32),
                pltpu.VMEM((quarter, hidden // 2), f32),
                dma((48,)), dma((56,)), dma((2,)), dma((4,)), dma((26,)), dma((24,)), dma((13,)), dma((13,)),
            ],
            compiler_params=pltpu.CompilerParams(collective_id=1, has_side_effects=True, vmem_limit_bytes=VMEM_BYTES),
            name='layer_two',
        )(adj_rows, h1, s1, pos, count, weight_two.T, weight_two, label_rows[None, :], mask_rows[None, :])

        dw_one = out[:feats]
        dw_two = out[pad:pad + classes].T
        loss = out[pad + classes, 0:1] / count[0, 0:1]
        return loss, dw_one, dw_two

    return jax.shard_map(local_step, mesh=mesh, in_specs=(P(AXIS, None), P(AXIS, None), P(None, None), P(None, None), P(AXIS), P(AXIS)), out_specs=(P(None), P(None, None), P(None, None)), check_vma=False)
```
